256 devices in a mesh: pole: 4 (over y), tile: 64 (over z, x, core).
Axes of the slice: x: 4, y: 4, z: 8, core: 2. Of those that a mesh axis runs over, the one named last changes fastest.
Arguments:
- state: float32 [3, 1024, 2048], P(None, 'tile', 'pole'), may hold values from -6 to 6
- depth: float32 [1024, 2048], P('tile', 'pole'), may hold values from 0.5 to 2
- pole_real: float32 [16], P('pole'), may hold values from -1.5 to -0.5
- pole_imag: float32 [16], P('pole'), may hold values from -2 to 2
- pole_weight: float32 [2, 16], P(None, 'pole'), may hold values from -3 to 3
Outputs:
- advanced: float32 [3, 1024, 2048], P(None, 'tile', 'pole')
The draws below stay inside these ranges and needn't reach their ends.
All inputs are finite; a program needn't handle non-finite values.
Results may differ from the reference program's by a relative error of at most 0.00002.
Values sent between devices are 32-bit elements; how exact they have to be, the bound alone decides.
A program may use at most 64 MiB of HBM per device.

```python
import jax
import jax.numpy as jnp

ITERS = 8
NX = 1024
NY = 2048
POLES = 16


def levels(key, dims, pieces, low, largest):
    level = 1.0
    for dim, shards_of in pieces:
        heights = jax.random.uniform(jax.random.fold_in(jax.random.fold_in(key, 6), dim), (shards_of,), jnp.float32, low / len(pieces), largest / len(pieces))
        level = level * jnp.repeat(jnp.exp(heights), dims[dim] // shards_of).reshape((-1,) + (1,) * (len(dims) - 1 - dim))
    return level


def noise(rng, dims, scale, reach, shards=(), kind=jnp.bfloat16):
    gain = levels(rng, dims, shards, -0.22, 0.18) if shards else 1.0
    values = jax.random.normal(rng, dims, jnp.float32) * scale * gain
    return jnp.minimum(jnp.maximum(values, -reach), reach).astype(kind)


def setup_inputs(seed: int = 0) -> dict:
    key_of = jax.random.split(jax.random.key(seed), 6)
    state = noise(key_of[0], (3, NX, NY), 1.0, 6.0, ((1, 64), (2, 4)), jnp.float32)
    depth = jnp.clip(0.5 + 1.5 * jax.random.uniform(key_of[1], (NX, NY), jnp.float32) ** levels(key_of[1], (NX, NY), ((0, 64), (1, 4)), -0.2, 0.2), 0.5, 2.0)
    pole_real = jnp.clip(-1.5 + 1.0 * jax.random.uniform(key_of[2], (POLES,), jnp.float32) ** levels(key_of[2], (POLES,), ((0, 4),), -0.2, 0.2), -1.5, -0.5)
    pole_imag = jnp.clip(jax.random.uniform(key_of[3], (POLES,), jnp.float32, -2.0, 2.0) * levels(key_of[3], (POLES,), ((0, 4),), -0.4, 0.0), -2.0, 2.0)
    pole_weight = noise(key_of[4], (2, POLES), 0.5, 3.0, ((1, 4),), jnp.float32)
    return dict(state=state, depth=depth, pole_real=pole_real, pole_imag=pole_imag, pole_weight=pole_weight)


coriolis = 0.7
centre = 8.0
half_width = 8.0


def complex_product(left_real, left_imaginary, right_real, right_imaginary):
    return (left_real * right_real - left_imaginary * right_imaginary,
            left_real * right_imaginary + left_imaginary * right_real)


def complex_quotient(top_real, top_imaginary, under_real, under_imaginary):
    norm = under_real * under_real + under_imaginary * under_imaginary
    return ((top_real * under_real + top_imaginary * under_imaginary) / norm,
            (top_imaginary * under_real - top_real * under_imaginary) / norm)


def chebyshev_table(alpha_real, alpha_imaginary):
    shift_real = alpha_real * alpha_real - alpha_imaginary * alpha_imaginary + coriolis * coriolis
    shift_imaginary = 2.0 * alpha_real * alpha_imaginary
    sigma_real = (shift_real + centre) / half_width
    sigma_imaginary = shift_imaginary / half_width
    unity = jnp.ones_like(sigma_real)
    nought = jnp.zeros_like(sigma_real)
    rho_real, rho_imaginary = complex_quotient(unity, nought, sigma_real, sigma_imaginary)
    table = []
    for index in range(ITERS - 1):
        next_real, next_imaginary = complex_quotient(unity, nought, 2.0 * sigma_real - rho_real, 2.0 * sigma_imaginary - rho_imaginary)
        keep_real, keep_imaginary = complex_product(next_real, next_imaginary, rho_real, rho_imaginary)
        table.append((keep_real, keep_imaginary, 2.0 * next_real / half_width, 2.0 * next_imaginary / half_width))
        rho_real, rho_imaginary = next_real, next_imaginary
    return shift_real, shift_imaginary, table


def advance(entry, search_real, search_imaginary, resid_real, resid_imaginary):
    first_real, first_imaginary = complex_product(entry[0], entry[1], search_real, search_imaginary)
    second_real, second_imaginary = complex_product(entry[2], entry[3], resid_real, resid_imaginary)
    return first_real + second_real, first_imaginary + second_imaginary


def row_slope(field):
    return 0.5 * (jnp.roll(field, -1, 0) - jnp.roll(field, 1, 0))


def column_slope(field):
    return 0.5 * (jnp.roll(field, -1, 1) - jnp.roll(field, 1, 1))


def periodic_stiffness(field, depth):
    east = 0.5 * (depth + jnp.roll(depth, -1, 0)) * (jnp.roll(field, -1, 0) - field)
    north = 0.5 * (depth + jnp.roll(depth, -1, 1)) * (jnp.roll(field, -1, 1) - field)
    return -(east - jnp.roll(east, 1, 0) + north - jnp.roll(north, 1, 1))


def reference(state, depth, pole_real, pole_imag, pole_weight):
    height = state[0]
    east_speed = state[1]
    north_speed = state[2]
    flux_div = row_slope(depth * east_speed) + column_slope(depth * north_speed)
    flux_curl = row_slope(depth * north_speed) - column_slope(depth * east_speed)
    shift_all_real, shift_all_imaginary, table_all = chebyshev_table(pole_real, pole_imag)
    out_height = jnp.zeros_like(height)
    out_east = jnp.zeros_like(height)
    out_north = jnp.zeros_like(height)
    for pole in range(POLES):
        alpha_real = pole_real[pole]
        alpha_imaginary = pole_imag[pole]
        shift_real = shift_all_real[pole]
        shift_imaginary = shift_all_imaginary[pole]
        top_real = shift_real * height - alpha_real * flux_div - coriolis * flux_curl
        top_imaginary = shift_imaginary * height - alpha_imaginary * flux_div
        rhs_real, rhs_imaginary = complex_quotient(top_real, top_imaginary, alpha_real, alpha_imaginary)
        resid_real, resid_imaginary = rhs_real, rhs_imaginary
        search_real, search_imaginary = complex_quotient(rhs_real, rhs_imaginary, shift_real + centre, shift_imaginary)
        iterate_real = jnp.zeros_like(rhs_real)
        iterate_imaginary = jnp.zeros_like(rhs_real)
        for index in range(ITERS):
            image_real = shift_real * search_real - shift_imaginary * search_imaginary + periodic_stiffness(search_real, depth)
            image_imaginary = shift_real * search_imaginary + shift_imaginary * search_real + periodic_stiffness(search_imaginary, depth)
            iterate_real = iterate_real + search_real
            iterate_imaginary = iterate_imaginary + search_imaginary
            resid_real = resid_real - image_real
            resid_imaginary = resid_imaginary - image_imaginary
            if index < ITERS - 1:
                entry = tuple(part[pole] for part in table_all[index])
                search_real, search_imaginary = advance(entry, search_real, search_imaginary, resid_real, resid_imaginary)
        weight_real = pole_weight[0, pole]
        weight_imaginary = pole_weight[1, pole]
        scale_real, scale_imaginary = complex_quotient(weight_real, weight_imaginary, shift_real, shift_imaginary)
        push_real = east_speed - row_slope(iterate_real)
        push_imaginary = -row_slope(iterate_imaginary)
        lift_real = north_speed - column_slope(iterate_real)
        lift_imaginary = -column_slope(iterate_imaginary)
        east_real, east_imaginary = complex_product(alpha_real, alpha_imaginary, push_real, push_imaginary)
        east_real = east_real + coriolis * lift_real
        east_imaginary = east_imaginary + coriolis * lift_imaginary
        north_real, north_imaginary = complex_product(alpha_real, alpha_imaginary, lift_real, lift_imaginary)
        north_real = north_real - coriolis * push_real
        north_imaginary = north_imaginary - coriolis * push_imaginary
        out_height = out_height + (weight_real * iterate_real - weight_imaginary * iterate_imaginary)
        out_east = out_east + (scale_real * east_real - scale_imaginary * east_imaginary)
        out_north = out_north + (scale_real * north_real - scale_imaginary * north_imaginary)
    return jnp.stack([out_height, out_east, out_north])
```

```python
import jax
import jax.numpy as jnp
from jax import lax
from jax.experimental import pallas as pl
from jax.experimental.pallas import tpu as pltpu
from jax.sharding import PartitionSpec as P

MESH = pl.DeviceIdType.MESH
ITERS = 8
CORIOLIS = 0.7
OWN = 16
ROWS = 3 * OWN
LANES = 128


def times(left, right):
    return (
        left[0] * right[0] - left[1] * right[1],
        left[0] * right[1] + left[1] * right[0],
    )


def inverse(value):
    norm = value[0] * value[0] + value[1] * value[1]
    return (value[0] / norm, -value[1] / norm)


def scaled(factor, value):
    return (factor * value[0], factor * value[1])


def coefficient_tile(real_ref, imag_ref, weight_ref, poles):
    lane = lax.broadcasted_iota(jnp.int32, (8, LANES), 1)
    row = lax.broadcasted_iota(jnp.int32, (8, LANES), 0)
    alpha = [jnp.full((8, LANES), -1.0, jnp.float32), jnp.zeros((8, LANES), jnp.float32)]
    beta = [jnp.zeros((8, LANES), jnp.float32)] * 2
    for k in range(poles):
        here = lane == k
        alpha[0] = jnp.where(here, real_ref[k], alpha[0])
        alpha[1] = jnp.where(here, imag_ref[k], alpha[1])
        beta[0] = jnp.where(here, weight_ref[0, k], beta[0])
        beta[1] = jnp.where(here, weight_ref[1, k], beta[1])
    square = times(alpha, alpha)
    shift = (square[0] + CORIOLIS * CORIOLIS, square[1])
    sigma = ((shift[0] + 8.0) * 0.125, shift[1] * 0.125)
    twice = scaled(2.0, sigma)
    second = [(jnp.ones_like(lane, jnp.float32), jnp.zeros_like(lane, jnp.float32)), twice]
    for _ in range(ITERS - 2):
        product = times(twice, second[-1])
        second.append((product[0] - second[-2][0], product[1] - second[-2][1]))
    product = times(sigma, second[7])
    last = (product[0] - second[6][0], product[1] - second[6][1])
    kappa = scaled(0.125, inverse(last))
    order_real, order_imag = second[7]
    for m in range(1, ITERS):
        order_real = jnp.where(row == m, 2.0 * second[7 - m][0], order_real)
        order_imag = jnp.where(row == m, 2.0 * second[7 - m][1], order_imag)
    over_alpha = inverse(alpha)
    gamma = times(beta, inverse(shift))
    gamma_alpha = times(gamma, alpha)
    weighted = times(kappa, beta)
    gammas = times(kappa, gamma)
    weighted_over = times(weighted, over_alpha)
    gammas_over = times(gammas, over_alpha)
    gammas_alpha = times(gammas, alpha)
    pieces = (
        times(weighted_over, shift),
        scaled(-1.0, weighted),
        scaled(-CORIOLIS, weighted_over),
        scaled(0.5, weighted),
        scaled(-0.5, gammas_alpha),
        scaled(-0.5 * CORIOLIS, gammas),
        scaled(0.5 * CORIOLIS, weighted_over),
        scaled(-0.5 * CORIOLIS, gammas),
        scaled(-0.5 * CORIOLIS * CORIOLIS, gammas_over),
    )
    sums = [piece[0] * order_real - piece[1] * order_imag for piece in pieces]
    sums += [gamma_alpha[0], CORIOLIS * gamma[0]]
    tile = jnp.zeros((8, LANES), jnp.float32)
    for index, value in enumerate(sums):
        tile = jnp.where(lane == index, jnp.sum(value, axis=1, keepdims=True), tile)
    return tile


def kernel(
    state_ref, depth_ref, real_ref, imag_ref, weight_ref, out_ref,
    block, edges, left_edges, right_edges, mine, theirs, table,
    real_s, imag_s, weight_s,
    flux, face, north, south, middle, chain, slope,
    load_sem, send_sem, recv_sem,
):
    poles = real_s.shape[0]
    tiles_of = state_ref.shape[2] // LANES
    p, t = lax.axis_index("pole"), lax.axis_index("tile")
    n_pole, n_tile = lax.axis_size("pole"), lax.axis_size("tile")
    peers_p = [lax.rem(p + d, n_pole) for d in range(n_pole)]
    right, left = peers_p[1], peers_p[n_pole - 1]
    down, up = lax.rem(t + 1, n_tile), lax.rem(t + n_tile - 1, n_tile)

    barrier = pltpu.get_barrier_semaphore()
    around = [(left, up), (p, up), (right, up), (left, t), (right, t), (left, down), (p, down), (right, down)]
    around += [(peers_p[d], t) for d in range(2, n_pole - 1)]
    for to in around:
        pl.semaphore_signal(barrier, inc=1, device_id=to, device_id_type=MESH)

    loads = [
        pltpu.make_async_copy(real_ref, real_s, load_sem.at[0]),
        pltpu.make_async_copy(imag_ref, imag_s, load_sem.at[1]),
        pltpu.make_async_copy(weight_ref, weight_s, load_sem.at[2]),
    ]
    for c in range(tiles_of):
        columns = pl.ds(c * LANES, LANES)
        loads.append(pltpu.make_async_copy(
            state_ref.at[:, :, columns], block.at[0:3, c, OWN:2 * OWN, :], load_sem.at[3 + 2 * c]))
        loads.append(pltpu.make_async_copy(
            depth_ref.at[:, columns], block.at[3, c, OWN:2 * OWN, :], load_sem.at[4 + 2 * c]))
    for copy in loads:
        copy.start()
    for copy in loads[3:]:
        copy.wait()

    lane = lax.broadcasted_iota(jnp.int32, (OWN, LANES), 1)
    group = ((lane + 16) // 32) % 4
    packed = jnp.zeros((OWN, LANES), jnp.float32)
    for f in range(4):
        piece = jnp.where(lane < 64, block[f, 0, OWN:2 * OWN, :], block[f, tiles_of - 1, OWN:2 * OWN, :])
        if f:
            piece = pltpu.roll(piece, 32 * f, 1)
        packed = jnp.where(group == f, piece, packed)
    edges[...] = packed

    pl.semaphore_wait(barrier, len(around))

    def remote(index, source, target, to):
        return pltpu.make_async_remote_copy(
            src_ref=source, dst_ref=target, send_sem=send_sem.at[index], recv_sem=recv_sem.at[index],
            device_id=to, device_id_type=MESH)

    own = pl.ds(0, tiles_of)
    sends = [
        remote(0, edges, left_edges.at[0:OWN, :], (right, down)),
        remote(1, edges, right_edges.at[0:OWN, :], (left, down)),
        remote(2, edges, left_edges.at[2 * OWN:ROWS, :], (right, up)),
        remote(3, edges, right_edges.at[2 * OWN:ROWS, :], (left, up)),
        remote(4, block.at[1:4, own, OWN:2 * OWN, :], block.at[1:4, own, 0:OWN, :], (p, down)),
        remote(5, block.at[1:4, own, OWN:2 * OWN, :], block.at[1:4, own, 2 * OWN:ROWS, :], (p, up)),
        remote(6, block.at[0, own, 24:32, :], block.at[0, own, 8:16, :], (p, down)),
        remote(7, block.at[0, own, 16:24, :], block.at[0, own, 32:40, :], (p, up)),
        remote(8, edges, left_edges.at[OWN:2 * OWN, :], (right, t)),
        remote(9, edges, right_edges.at[OWN:2 * OWN, :], (left, t)),
    ]
    for copy in sends:
        copy.start()

    for copy in loads[:3]:
        copy.wait()
    mine[...] = coefficient_tile(real_s, imag_s, weight_s, poles)
    totals = [
        remote(9 + d, mine, theirs.at[d - 1], (peers_p[d], t)) for d in range(1, n_pole)
    ]
    for copy in totals:
        copy.start()

    for copy in sends:
        copy.wait_recv()

    halo = tiles_of
    tiles = tiles_of + 1
    wide_lane = lax.broadcasted_iota(jnp.int32, (ROWS, LANES), 1)
    both = jnp.where(wide_lane % 32 >= 16, left_edges[...], right_edges[...])
    for f in range(4):
        block[f, halo, :, :] = pltpu.roll(both, (LANES - 32 * f) % LANES, 1)

    def eastward(pieces):
        edge = lax.broadcasted_iota(jnp.int32, pieces[0].shape, 1) == LANES - 1
        turned = [pltpu.roll(piece, LANES - 1, 1) for piece in pieces]
        return [jnp.where(edge, turned[(c + 1) % tiles], turned[c]) for c in range(tiles)]

    def westward(pieces):
        edge = lax.broadcasted_iota(jnp.int32, pieces[0].shape, 1) == 0
        turned = [pltpu.roll(piece, 1, 1) for piece in pieces]
        return [jnp.where(edge, turned[(c - 1) % tiles], turned[c]) for c in range(tiles)]

    every = range(tiles)
    for c in every:
        face[c, 0:40, :] = (block[3, c, 0:40, :] + block[3, c, 1:41, :]) * 0.125
        flux[0, c, :, :] = block[3, c, :, :] * block[1, c, :, :]
        flux[1, c, :, :] = block[3, c, :, :] * block[2, c, :, :]
        chain[0, 0, c, 8:40, :] = block[0, c, 8:40, :]
    here = [block[3, c, 8:40, :] for c in every]
    beside = eastward(here)
    to_north = [(here[c] + beside[c]) * 0.125 for c in every]
    to_south = westward(to_north)
    for c in every:
        north[c, :, :] = to_north[c]
        south[c, :, :] = to_south[c]
        middle[c, :, :] = 2.0 - (face[c, 8:40, :] + face[c, 7:39, :] + to_north[c] + to_south[c])
    for which in range(2):
        here = [flux[which, c, 8:40, :] for c in every]
        after, before = eastward(here), westward(here)
        for c in every:
            along = 0.5 * (flux[which, c, 9:41, :] - flux[which, c, 7:39, :])
            across = 0.5 * (after[c] - before[c])
            if which == 0:
                chain[0, 1, c, 8:40, :] = along
                chain[0, 2, c, 8:40, :] = -across
            else:
                chain[0, 1, c, 8:40, :] = chain[0, 1, c, 8:40, :] + across
                chain[0, 2, c, 8:40, :] = chain[0, 2, c, 8:40, :] + along

    for m in range(ITERS - 1):
        first, length = (8, 32) if m < 3 else (12, 24)
        rows = slice(first, first + length)
        for f in range(3):
            here = [chain[m, f, c, rows, :] for c in every]
            after, before = eastward(here), westward(here)
            for c in every:
                inner = slice(first - 8, first - 8 + length)
                value = (
                    middle[c, inner, :] * here[c]
                    + face[c, rows, :] * chain[m, f, c, first + 1:first + 1 + length, :]
                    + face[c, first - 1:first - 1 + length, :] * chain[m, f, c, first - 1:first - 1 + length, :]
                    + north[c, inner, :] * after[c]
                    + south[c, inner, :] * before[c]
                )
                if m == 0:
                    value = 0.5 * value
                else:
                    value = value - chain[m - 1, f, c, rows, :]
                chain[m + 1, f, c, rows, :] = value

    for copy in totals:
        copy.wait_recv()
    total = mine[...]
    for d in range(n_pole - 1):
        total = total + theirs[d]
    for index in range(11):
        table[index, :, :] = jnp.broadcast_to(total[:, index:index + 1], (8, LANES))

    for c in every:
        height = jnp.zeros((OWN, LANES), jnp.float32)
        push = jnp.zeros((24, LANES), jnp.float32)
        lift = jnp.zeros((24, LANES), jnp.float32)
        for m in range(ITERS):
            for f in range(3):
                wide = chain[m, f, c, 15:39, :]
                push = push + table[3 + f, m:m + 1, :] * wide
                lift = lift + table[6 + f, m:m + 1, :] * wide
                if c < tiles_of:
                    height = height + table[f, m:m + 1, :] * chain[m, f, c, 16:32, :]
        slope[0, c, :, :] = push
        slope[1, c, :, :] = lift
        if c < tiles_of:
            out_ref[0, :, c * LANES:(c + 1) * LANES] = height
    keep_first, keep_second = table[9, 0:1, :], table[10, 0:1, :]
    here = [slope[0, c, 1:17, :] for c in every]
    push_after, push_before = eastward(here), westward(here)
    here = [slope[1, c, 1:17, :] for c in every]
    lift_after, lift_before = eastward(here), westward(here)
    for c in range(tiles_of):
        columns = slice(c * LANES, (c + 1) * LANES)
        east, north_speed = block[1, c, OWN:2 * OWN, :], block[2, c, OWN:2 * OWN, :]
        push_along = slope[0, c, 2:18, :] - slope[0, c, 0:16, :]
        lift_along = slope[1, c, 2:18, :] - slope[1, c, 0:16, :]
        out_ref[1, :, columns] = (
            keep_first * east + keep_second * north_speed
            - push_along - (lift_after[c] - lift_before[c]))
        out_ref[2, :, columns] = (
            keep_first * north_speed - keep_second * east
            - (push_after[c] - push_before[c]) + lift_along)

    for copy in sends + totals:
        copy.wait_send()


def shards(state, depth, pole_real, pole_imag, pole_weight):
    fields, rows, columns = state.shape
    poles = pole_real.shape[0]
    tiles = columns // LANES + 1
    n_pole = lax.axis_size("pole")
    copies = 10 + n_pole - 1
    f32 = jnp.float32
    return pl.pallas_call(
        kernel,
        out_shape=jax.ShapeDtypeStruct((3, rows, columns), f32),
        in_specs=[pl.BlockSpec(memory_space=pl.ANY)] * 5,
        out_specs=pl.BlockSpec(memory_space=pltpu.VMEM),
        scratch_shapes=[
            pltpu.VMEM((4, tiles, ROWS, LANES), f32),
            pltpu.VMEM((OWN, LANES), f32),
            pltpu.VMEM((ROWS, LANES), f32),
            pltpu.VMEM((ROWS, LANES), f32),
            pltpu.VMEM((8, LANES), f32),
            pltpu.VMEM((n_pole - 1, 8, LANES), f32),
            pltpu.VMEM((11, 8, LANES), f32),
            pltpu.SMEM((poles,), f32),
            pltpu.SMEM((poles,), f32),
            pltpu.SMEM((2, poles), f32),
            pltpu.VMEM((2, tiles, ROWS, LANES), f32),
            pltpu.VMEM((tiles, ROWS, LANES), f32),
            pltpu.VMEM((tiles, 32, LANES), f32),
            pltpu.VMEM((tiles, 32, LANES), f32),
            pltpu.VMEM((tiles, 32, LANES), f32),
            pltpu.VMEM((ITERS, 3, tiles, ROWS, LANES), f32),
            pltpu.VMEM((2, tiles, 24, LANES), f32),
            pltpu.SemaphoreType.DMA((3 + 2 * (tiles - 1),)),
            pltpu.SemaphoreType.DMA((copies,)),
            pltpu.SemaphoreType.DMA((copies,)),
        ],
        compiler_params=pltpu.CompilerParams(collective_id=0, has_side_effects=True),
        name="rexi_step",
    )(state, depth, pole_real, pole_imag, pole_weight)


def solution(mesh):
    return jax.shard_map(
        shards,
        mesh=mesh,
        in_specs=(
            P(None, "tile", "pole"),
            P("tile", "pole"),
            P("pole"),
            P("pole"),
            P(None, "pole"),
        ),
        out_specs=P(None, "tile", "pole"),
        check_vma=False,
    )
```

```python
import jax
import jax.numpy as jnp
from jax import lax
from jax.experimental import pallas as pl
from jax.experimental.pallas import tpu as pltpu
from jax.sharding import PartitionSpec as P

MESH = pl.DeviceIdType.MESH
ITERS = 8
CORIOLIS = 0.7
OWN = 16
ROWS = 3 * OWN
LANES = 128
PLANE = 8
STEPS = ((0, 1), (1, 1), (-1, 1), (1, 0), (-1, 0), (0, -1), (1, -1), (-1, -1), (2, 0))
OPPOSITE = (5, 7, 6, 4, 3, 0, 2, 1, 8)


def times(left, right):
    return (
        left[0] * right[0] - left[1] * right[1],
        left[0] * right[1] + left[1] * right[0],
    )


def inverse(value):
    norm = value[0] * value[0] + value[1] * value[1]
    return (value[0] / norm, -value[1] / norm)


def scaled(factor, value):
    return (factor * value[0], factor * value[1])


def coefficient_tile(real_ref, imag_ref, weight_ref, poles):
    lane = lax.broadcasted_iota(jnp.int32, (8, LANES), 1)
    row = lax.broadcasted_iota(jnp.int32, (8, LANES), 0)
    alpha = [jnp.full((8, LANES), -1.0, jnp.float32), jnp.zeros((8, LANES), jnp.float32)]
    beta = [jnp.zeros((8, LANES), jnp.float32)] * 2
    for k in range(poles):
        here = lane == k
        alpha[0] = jnp.where(here, real_ref[k], alpha[0])
        alpha[1] = jnp.where(here, imag_ref[k], alpha[1])
        beta[0] = jnp.where(here, weight_ref[0, k], beta[0])
        beta[1] = jnp.where(here, weight_ref[1, k], beta[1])
    square = times(alpha, alpha)
    shift = (square[0] + CORIOLIS * CORIOLIS, square[1])
    sigma = ((shift[0] + 8.0) * 0.125, shift[1] * 0.125)
    twice = scaled(2.0, sigma)
    second = [(jnp.ones_like(lane, jnp.float32), jnp.zeros_like(lane, jnp.float32)), twice]
    for _ in range(ITERS - 2):
        product = times(twice, second[-1])
        second.append((product[0] - second[-2][0], product[1] - second[-2][1]))
    product = times(sigma, second[7])
    last = (product[0] - second[6][0], product[1] - second[6][1])
    kappa = scaled(0.125, inverse(last))
    order_real, order_imag = second[7]
    for m in range(1, ITERS):
        order_real = jnp.where(row == m, 2.0 * second[7 - m][0], order_real)
        order_imag = jnp.where(row == m, 2.0 * second[7 - m][1], order_imag)
    over_alpha = inverse(alpha)
    gamma = times(beta, inverse(shift))
    gamma_alpha = times(gamma, alpha)
    weighted = times(kappa, beta)
    gammas = times(kappa, gamma)
    weighted_over = times(weighted, over_alpha)
    gammas_over = times(gammas, over_alpha)
    gammas_alpha = times(gammas, alpha)
    pieces = (
        times(weighted_over, shift),
        scaled(-1.0, weighted),
        scaled(-CORIOLIS, weighted_over),
        scaled(0.5, weighted),
        scaled(-0.5, gammas_alpha),
        scaled(-0.5 * CORIOLIS, gammas),
        scaled(0.5 * CORIOLIS, weighted_over),
        scaled(-0.5 * CORIOLIS, gammas),
        scaled(-0.5 * CORIOLIS * CORIOLIS, gammas_over),
    )
    sums = [piece[0] * order_real - piece[1] * order_imag for piece in pieces]
    sums += [gamma_alpha[0], CORIOLIS * gamma[0]]
    tile = jnp.zeros((8, LANES), jnp.float32)
    for index, value in enumerate(sums):
        tile = jnp.where(lane == index, jnp.sum(value, axis=1, keepdims=True), tile)
    return tile


def waits_for(step, p, t, n_pole, n_tile):
    dp, dt = step
    last = t == n_tile - 1
    if dt < 0:
        return jnp.logical_or(t == 0, last)
    if dt > 0:
        return None
    return jnp.logical_and(last, {1: p != n_pole - 1, -1: p == 0, 2: p < n_pole // 2}[dp])


def heard_later(step, p, t, n_pole, n_tile):
    dp, dt = step
    last = t == n_tile - 1
    if dt > 0:
        return jnp.logical_or(last, t == n_tile - 2)
    if dt < 0:
        return None
    return jnp.logical_and(last, {1: p == n_pole - 1, -1: p != 0, 2: p >= n_pole // 2}[dp])


def kernel(
    state_ref, depth_ref, real_ref, imag_ref, weight_ref, out_ref,
    block, edges, left_edges, right_edges, mine, theirs, table,
    real_s, imag_s, weight_s,
    flux, face, north, south, middle, chain, slope,
    load_sem, send_sem, recv_sem, ready_sem,
):
    poles = real_s.shape[0]
    tiles_of = state_ref.shape[2] // LANES
    p, t = lax.axis_index("pole"), lax.axis_index("tile")
    n_pole, n_tile = lax.axis_size("pole"), lax.axis_size("tile")
    peers = [(lax.rem(p + dp + n_pole, n_pole), lax.rem(t + dt + n_tile, n_tile)) for dp, dt in STEPS]
    early = [waits_for(step, p, t, n_pole, n_tile) for step in STEPS]
    late = [heard_later(step, p, t, n_pole, n_tile) for step in STEPS]

    loads = [
        pltpu.make_async_copy(real_ref, real_s, load_sem.at[0]),
        pltpu.make_async_copy(imag_ref, imag_s, load_sem.at[1]),
        pltpu.make_async_copy(weight_ref, weight_s, load_sem.at[2]),
    ]
    for c in range(tiles_of):
        columns = pl.ds(c * LANES, LANES)
        loads.append(pltpu.make_async_copy(
            state_ref.at[:, :, columns], block.at[0:3, c, OWN:2 * OWN, :], load_sem.at[3 + 2 * c]))
        loads.append(pltpu.make_async_copy(
            depth_ref.at[:, columns], block.at[3, c, OWN:2 * OWN, :], load_sem.at[4 + 2 * c]))
    for copy in loads[3:] + loads[:3]:
        copy.start()

    barrier = pltpu.get_barrier_semaphore()
    expected = jnp.int32(len(STEPS))
    for k, to in enumerate(peers):
        if early[k] is not None:
            expected = expected - early[k].astype(jnp.int32)

        def greet(to=to):
            pl.semaphore_signal(barrier, inc=1, device_id=to, device_id_type=MESH)
        if late[k] is None:
            greet()
        else:
            pl.when(jnp.logical_not(late[k]))(greet)
    pl.semaphore_wait(barrier, expected)
    for k, to in enumerate(peers):
        if late[k] is not None:
            @pl.when(late[k])
            def answer(k=k, to=to):
                pl.semaphore_signal(ready_sem.at[OPPOSITE[k]], inc=1, device_id=to, device_id_type=MESH)

    def remote(index, source, target, to):
        return pltpu.make_async_remote_copy(
            src_ref=source, dst_ref=target, send_sem=send_sem.at[index], recv_sem=recv_sem.at[index],
            device_id=to, device_id_type=MESH)

    own = pl.ds(0, tiles_of)
    lower, upper = slice(23, 32), slice(16, 25)
    above, below = slice(7, 16), slice(32, 41)
    sends = [
        remote(0, block.at[:, own, lower, :], block.at[:, own, above, :], peers[0]),
        remote(1, edges.at[7:16, :], left_edges.at[above, :], peers[1]),
        remote(2, edges.at[7:16, :], right_edges.at[above, :], peers[2]),
        remote(3, edges, left_edges.at[OWN:2 * OWN, :], peers[3]),
        remote(4, edges, right_edges.at[OWN:2 * OWN, :], peers[4]),
        remote(5, block.at[:, own, upper, :], block.at[:, own, below, :], peers[5]),
        remote(6, edges.at[0:9, :], left_edges.at[below, :], peers[6]),
        remote(7, edges.at[0:9, :], right_edges.at[below, :], peers[7]),
    ]
    from_above, from_side, from_under = sends[0:3], sends[3:5], sends[5:8]
    from_below = from_side + from_under
    totals = [
        remote(8, mine, theirs.at[0], peers[3]),
        remote(9, mine, theirs.at[1], peers[4]),
        remote(10, mine, theirs.at[2], peers[8]),
    ]

    for copy in loads[3:]:
        copy.wait()
    lane = lax.broadcasted_iota(jnp.int32, (OWN, LANES), 1)
    group = ((lane + 16) // 32) % 4
    packed = jnp.zeros((OWN, LANES), jnp.float32)
    for f in range(4):
        piece = jnp.where(lane < 64, block[f, 0, OWN:2 * OWN, :], block[f, tiles_of - 1, OWN:2 * OWN, :])
        if f:
            piece = pltpu.roll(piece, 32 * f, 1)
        packed = jnp.where(group == f, piece, packed)
    edges[...] = packed
    for k in (1, 2, 0, 3, 4, 6, 7, 5):
        if early[k] is None:
            sends[k].start()
        else:
            pl.when(jnp.logical_not(early[k]))(sends[k].start)

    for copy in loads[:3]:
        copy.wait()
    mine[...] = coefficient_tile(real_s, imag_s, weight_s, poles)
    for k, copy in ((3, totals[0]), (4, totals[1]), (8, totals[2])):
        pl.when(jnp.logical_not(early[k]))(copy.start)

    @pl.when(t == n_tile - 1)
    def _():
        for k, copies in ((5, sends[5:6]), (6, sends[6:7]), (7, sends[7:8]),
                          (3, [sends[3], totals[0]]), (4, [sends[4], totals[1]]), (8, totals[2:])):
            def send(k=k, copies=copies):
                pl.semaphore_wait(ready_sem.at[k], 1)
                for copy in copies:
                    copy.start()
            if k in (5, 6, 7):
                send()
            else:
                pl.when(early[k])(send)

    halo = tiles_of
    tiles = tiles_of + 1
    every = range(tiles)

    def eastward(pieces):
        edge = lax.broadcasted_iota(jnp.int32, pieces[0].shape, 1) == LANES - 1
        turned = [pltpu.roll(piece, LANES - 1, 1) for piece in pieces]
        return [jnp.where(edge, turned[(c + 1) % tiles], turned[c]) for c in every]

    def westward(pieces):
        edge = lax.broadcasted_iota(jnp.int32, pieces[0].shape, 1) == 0
        turned = [pltpu.roll(piece, 1, 1) for piece in pieces]
        return [jnp.where(edge, turned[(c - 1) % tiles], turned[c]) for c in every]

    def fields(m, f, c, rows):
        return chain[m, f, c, rows, :]

    def prepare(fresh, faces, columns_of, work):
        wide_lane = lax.broadcasted_iota(jnp.int32, (fresh.stop - fresh.start, LANES), 1)
        both = jnp.where(wide_lane % 32 >= 16, left_edges[fresh, :], right_edges[fresh, :])
        for f in range(4):
            block[f, halo, fresh, :] = pltpu.roll(both, (LANES - 32 * f) % LANES, 1) if f else both
        after_rows = slice(work.start + 1, work.stop + 1)
        before_rows = slice(work.start - 1, work.stop - 1)
        for c in every:
            chain[0, 0, c, fresh, :] = block[0, c, fresh, :]
            flux[0, c, fresh, :] = block[3, c, fresh, :] * block[1, c, fresh, :]
            flux[1, c, fresh, :] = block[3, c, fresh, :] * block[2, c, fresh, :]
        for c in every:
            face[c, faces, :] = (block[3, c, faces, :] + block[3, c, faces.start + 1:faces.stop + 1, :]) * 0.125
        here = [block[3, c, columns_of, :] for c in every]
        beside = eastward(here)
        to_north = [(here[c] + beside[c]) * 0.125 for c in every]
        to_south = westward(to_north)
        for c in every:
            north[c, columns_of, :] = to_north[c]
            south[c, columns_of, :] = to_south[c]
        for c in every:
            middle[c, work, :] = 2.0 - (
                face[c, work, :] + face[c, before_rows, :] + north[c, work, :] + south[c, work, :])
        here = [flux[0, c, work, :] for c in every]
        after, before = eastward(here), westward(here)
        here = [flux[1, c, work, :] for c in every]
        after_two, before_two = eastward(here), westward(here)
        for c in every:
            along = flux[0, c, after_rows, :] - flux[0, c, before_rows, :]
            along_two = flux[1, c, after_rows, :] - flux[1, c, before_rows, :]
            chain[0, 1, c, work, :] = 0.5 * (along + (after_two[c] - before_two[c]))
            chain[0, 2, c, work, :] = 0.5 * (along_two - (after[c] - before[c]))

    def advance(m, rows):
        after_rows = slice(rows.start + 1, rows.stop + 1)
        before_rows = slice(rows.start - 1, rows.stop - 1)
        for f in range(3):
            here = [fields(m, f, c, rows) for c in every]
            after, before = eastward(here), westward(here)
            for c in every:
                value = (
                    middle[c, rows, :] * here[c]
                    + face[c, rows, :] * fields(m, f, c, after_rows)
                    + face[c, before_rows, :] * fields(m, f, c, before_rows)
                    + north[c, rows, :] * after[c]
                    + south[c, rows, :] * before[c]
                )
                if m == 0:
                    value = 0.5 * value
                else:
                    value = value - fields(m - 1, f, c, rows)
                chain[m + 1, f, c, rows, :] = value

    def combine(wide, inner):
        for c in every:
            rows = wide if c < tiles_of else inner
            height = push = lift = None
            for m in range(ITERS):
                for f in range(3):
                    value = fields(m, f, c, rows)
                    one, two = table[3 + f, m:m + 1, :] * value, table[6 + f, m:m + 1, :] * value
                    push, lift = (one, two) if push is None else (push + one, lift + two)
                    if c < tiles_of:
                        part = table[f, m:m + 1, :] * fields(m, f, c, inner)
                        height = part if height is None else height + part
            slope[0, c, rows, :] = push
            slope[1, c, rows, :] = lift
            if c < tiles_of:
                out_ref[0, inner.start - OWN:inner.stop - OWN, c * LANES:(c + 1) * LANES] = height

    def spread_totals():
        for copy in totals:
            copy.wait_recv()
        total = mine[...]
        for d in range(n_pole - 1):
            total = total + theirs[d]
        for index in range(11):
            table[index, :, :] = jnp.broadcast_to(total[:, index:index + 1], (8, LANES))

    first_of_plane = lax.rem(t, PLANE) == 0

    @pl.when(first_of_plane)
    def _():
        for copy in from_below:
            copy.wait_recv()
        prepare(slice(16, 48), slice(16, 40), slice(16, 40), slice(16, 40))
        for m in range(ITERS - 1):
            advance(m, slice(16, 40) if m < 3 else slice(20, 36))
        spread_totals()
        combine(slice(24, 40), slice(24, 32))

        @pl.when(t == 0)
        def _():
            def answered(k):
                pl.semaphore_wait(ready_sem.at[k], 1)
                sends[k].start()
            pl.when(p == n_pole - 1)(lambda: answered(6))
            pl.when(p != 0)(lambda: answered(7))
            answered(5)
            pl.when(p != n_pole - 1)(lambda: answered(6))
            pl.when(p == 0)(lambda: answered(7))
        for copy in from_above:
            copy.wait_recv()
        prepare(slice(0, 16), slice(7, 16), slice(8, 16), slice(8, 24))
        for m in range(ITERS - 1):
            advance(m, slice(8, 24))
        combine(slice(8, 24), slice(16, 24))

    @pl.when(jnp.logical_not(first_of_plane))
    def _():
        for copy in from_above + from_side:
            copy.wait_recv()
        prepare(slice(0, 32), slice(7, 31), slice(8, 32), slice(8, 32))
        for m in range(ITERS - 1):
            advance(m, slice(8, 32) if m < 3 else slice(12, 28))
        spread_totals()
        combine(slice(8, 24), slice(16, 24))
        for copy in from_under:
            copy.wait_recv()
        prepare(slice(32, 48), slice(31, 39), slice(32, 40), slice(24, 40))
        for m in range(ITERS - 1):
            advance(m, slice(24, 40))
        combine(slice(24, 40), slice(24, 32))

    rows = slice(OWN, 2 * OWN)
    keep_first, keep_second = table[9, 0:1, :], table[10, 0:1, :]
    here = [slope[0, c, rows, :] for c in every]
    push_after, push_before = eastward(here), westward(here)
    here = [slope[1, c, rows, :] for c in every]
    lift_after, lift_before = eastward(here), westward(here)
    for c in range(tiles_of):
        columns = slice(c * LANES, (c + 1) * LANES)
        east, north_speed = block[1, c, rows, :], block[2, c, rows, :]
        push_along = slope[0, c, OWN + 1:2 * OWN + 1, :] - slope[0, c, OWN - 1:2 * OWN - 1, :]
        lift_along = slope[1, c, OWN + 1:2 * OWN + 1, :] - slope[1, c, OWN - 1:2 * OWN - 1, :]
        out_ref[1, :, columns] = (
            keep_first * east + keep_second * north_speed
            - push_along - (lift_after[c] - lift_before[c]))
        out_ref[2, :, columns] = (
            keep_first * north_speed - keep_second * east
            - (push_after[c] - push_before[c]) + lift_along)

    for copy in sends + totals:
        copy.wait_send()


def shards(state, depth, pole_real, pole_imag, pole_weight):
    fields, rows, columns = state.shape
    poles = pole_real.shape[0]
    tiles = columns // LANES + 1
    n_pole = lax.axis_size("pole")
    f32 = jnp.float32
    return pl.pallas_call(
        kernel,
        out_shape=pltpu.VMEM((3, rows, columns), f32),
        in_specs=[pl.BlockSpec(memory_space=pl.ANY)] * 5,
        out_specs=pl.BlockSpec(memory_space=pltpu.VMEM),
        scratch_shapes=[
            pltpu.VMEM((4, tiles, ROWS, LANES), f32),
            pltpu.VMEM((OWN, LANES), f32),
            pltpu.VMEM((ROWS, LANES), f32),
            pltpu.VMEM((ROWS, LANES), f32),
            pltpu.VMEM((8, LANES), f32),
            pltpu.VMEM((n_pole - 1, 8, LANES), f32),
            pltpu.VMEM((11, 8, LANES), f32),
            pltpu.SMEM((poles,), f32),
            pltpu.SMEM((poles,), f32),
            pltpu.SMEM((2, poles), f32),
            pltpu.VMEM((2, tiles, ROWS, LANES), f32),
            pltpu.VMEM((tiles, ROWS, LANES), f32),
            pltpu.VMEM((tiles, ROWS, LANES), f32),
            pltpu.VMEM((tiles, ROWS, LANES), f32),
            pltpu.VMEM((tiles, ROWS, LANES), f32),
            pltpu.VMEM((ITERS, 3, tiles, ROWS, LANES), f32),
            pltpu.VMEM((2, tiles, ROWS, LANES), f32),
            pltpu.SemaphoreType.DMA((3 + 2 * (tiles - 1),)),
            pltpu.SemaphoreType.DMA((11,)),
            pltpu.SemaphoreType.DMA((11,)),
            pltpu.SemaphoreType.REGULAR((len(STEPS),)),
        ],
        compiler_params=pltpu.CompilerParams(collective_id=0, has_side_effects=True),
        name="rexi_step",
    )(state, depth, pole_real, pole_imag, pole_weight)


def solution(mesh):
    return jax.shard_map(
        shards,
        mesh=mesh,
        in_specs=(
            P(None, "tile", "pole"),
            P("tile", "pole"),
            P("pole"),
            P("pole"),
            P(None, "pole"),
        ),
        out_specs=P(None, "tile", "pole"),
        check_vma=False,
    )
```

```python
import jax
import jax.numpy as jnp
from jax import lax
from jax.experimental import pallas as pl
from jax.experimental.pallas import tpu as pltpu
from jax.sharding import PartitionSpec as P

MESH = pl.DeviceIdType.MESH
ITERS = 8
CORIOLIS = 0.7
OWN = 16
ROWS = 3 * OWN
LANES = 128
PLANE = 8
STEPS = ((0, 1), (1, 1), (-1, 1), (1, 0), (-1, 0), (0, -1), (1, -1), (-1, -1), (2, 0))
OPPOSITE = (5, 7, 6, 4, 3, 0, 2, 1, 8)


def times(left, right):
    return (
        left[0] * right[0] - left[1] * right[1],
        left[0] * right[1] + left[1] * right[0],
    )


def inverse(value):
    norm = value[0] * value[0] + value[1] * value[1]
    return (value[0] / norm, -value[1] / norm)


def scaled(factor, value):
    return (factor * value[0], factor * value[1])


def coefficient_tile(real_ref, imag_ref, weight_ref, poles):
    lane = lax.broadcasted_iota(jnp.int32, (8, LANES), 1)
    row = lax.broadcasted_iota(jnp.int32, (8, LANES), 0)
    alpha = [jnp.full((8, LANES), -1.0, jnp.float32), jnp.zeros((8, LANES), jnp.float32)]
    beta = [jnp.zeros((8, LANES), jnp.float32)] * 2
    for k in range(poles):
        here = lane == k
        alpha[0] = jnp.where(here, real_ref[k], alpha[0])
        alpha[1] = jnp.where(here, imag_ref[k], alpha[1])
        beta[0] = jnp.where(here, weight_ref[0, k], beta[0])
        beta[1] = jnp.where(here, weight_ref[1, k], beta[1])
    square = times(alpha, alpha)
    shift = (square[0] + CORIOLIS * CORIOLIS, square[1])
    sigma = ((shift[0] + 8.0) * 0.125, shift[1] * 0.125)
    twice = scaled(2.0, sigma)
    second = [(jnp.ones_like(lane, jnp.float32), jnp.zeros_like(lane, jnp.float32)), twice]
    for _ in range(ITERS - 2):
        product = times(twice, second[-1])
        second.append((product[0] - second[-2][0], product[1] - second[-2][1]))
    product = times(sigma, second[7])
    last = (product[0] - second[6][0], product[1] - second[6][1])
    kappa = scaled(0.125, inverse(last))
    order_real, order_imag = second[7]
    for m in range(1, ITERS):
        order_real = jnp.where(row == m, 2.0 * second[7 - m][0], order_real)
        order_imag = jnp.where(row == m, 2.0 * second[7 - m][1], order_imag)
    over_alpha = inverse(alpha)
    gamma = times(beta, inverse(shift))
    gamma_alpha = times(gamma, alpha)
    weighted = times(kappa, beta)
    gammas = times(kappa, gamma)
    weighted_over = times(weighted, over_alpha)
    gammas_over = times(gammas, over_alpha)
    gammas_alpha = times(gammas, alpha)
    pieces = (
        times(weighted_over, shift),
        scaled(-1.0, weighted),
        scaled(-CORIOLIS, weighted_over),
        scaled(0.5, weighted),
        scaled(-0.5, gammas_alpha),
        scaled(-0.5 * CORIOLIS, gammas),
        scaled(0.5 * CORIOLIS, weighted_over),
        scaled(-0.5 * CORIOLIS, gammas),
        scaled(-0.5 * CORIOLIS * CORIOLIS, gammas_over),
    )
    sums = [piece[0] * order_real - piece[1] * order_imag for piece in pieces]
    sums += [gamma_alpha[0], CORIOLIS * gamma[0]]
    tile = jnp.zeros((8, LANES), jnp.float32)
    for index, value in enumerate(sums):
        tile = jnp.where(lane == index, jnp.sum(value, axis=1, keepdims=True), tile)
    return tile


def waits_for(step, p, t, n_pole, n_tile):
    dp, dt = step
    last = t == n_tile - 1
    if dt < 0:
        return jnp.logical_or(t == 0, last)
    if dt > 0:
        return None
    return jnp.logical_and(last, {1: p != n_pole - 1, -1: p == 0, 2: p < n_pole // 2}[dp])


def heard_later(step, p, t, n_pole, n_tile):
    dp, dt = step
    last = t == n_tile - 1
    if dt > 0:
        return jnp.logical_or(last, t == n_tile - 2)
    if dt < 0:
        return None
    return jnp.logical_and(last, {1: p == n_pole - 1, -1: p != 0, 2: p >= n_pole // 2}[dp])


def kernel(
    state_ref, depth_ref, real_ref, imag_ref, weight_ref, out_ref,
    block, edges, left_edges, right_edges, mine, theirs, table,
    real_s, imag_s, weight_s,
    flux, face, north, south, middle, chain, slope, gain, beyond,
    load_sem, send_sem, recv_sem, ready_sem,
):
    poles = real_s.shape[0]
    tiles_of = state_ref.shape[2] // LANES
    p, t = lax.axis_index("pole"), lax.axis_index("tile")
    n_pole, n_tile = lax.axis_size("pole"), lax.axis_size("tile")
    peers = [(lax.rem(p + dp + n_pole, n_pole), lax.rem(t + dt + n_tile, n_tile)) for dp, dt in STEPS]
    early = [waits_for(step, p, t, n_pole, n_tile) for step in STEPS]
    late = [heard_later(step, p, t, n_pole, n_tile) for step in STEPS]

    loads = [
        pltpu.make_async_copy(real_ref, real_s, load_sem.at[0]),
        pltpu.make_async_copy(imag_ref, imag_s, load_sem.at[1]),
        pltpu.make_async_copy(weight_ref, weight_s, load_sem.at[2]),
    ]
    for c in range(tiles_of):
        columns = pl.ds(c * LANES, LANES)
        loads.append(pltpu.make_async_copy(
            state_ref.at[:, :, columns], block.at[0:3, c, OWN:2 * OWN, :], load_sem.at[3 + 2 * c]))
        loads.append(pltpu.make_async_copy(
            depth_ref.at[:, columns], block.at[3, c, OWN:2 * OWN, :], load_sem.at[4 + 2 * c]))
    for copy in loads[3:] + loads[:3]:
        copy.start()

    barrier = pltpu.get_barrier_semaphore()
    expected = jnp.int32(len(STEPS))
    for k, to in enumerate(peers):
        if early[k] is not None:
            expected = expected - early[k].astype(jnp.int32)

        def greet(to=to):
            pl.semaphore_signal(barrier, inc=1, device_id=to, device_id_type=MESH)
        if late[k] is None:
            greet()
        else:
            pl.when(jnp.logical_not(late[k]))(greet)
    pl.semaphore_wait(barrier, expected)
    for k, to in enumerate(peers):
        if late[k] is not None:
            @pl.when(late[k])
            def answer(k=k, to=to):
                pl.semaphore_signal(ready_sem.at[OPPOSITE[k]], inc=1, device_id=to, device_id_type=MESH)

    def remote(index, source, target, to):
        return pltpu.make_async_remote_copy(
            src_ref=source, dst_ref=target, send_sem=send_sem.at[index], recv_sem=recv_sem.at[index],
            device_id=to, device_id_type=MESH)

    own = pl.ds(0, tiles_of)
    lower, upper = slice(23, 32), slice(16, 25)
    above, below = slice(7, 16), slice(32, 41)
    sends = [
        remote(0, block.at[:, own, lower, :], block.at[:, own, above, :], peers[0]),
        remote(1, edges.at[7:16, :], left_edges.at[above, :], peers[1]),
        remote(2, edges.at[7:16, :], right_edges.at[above, :], peers[2]),
        remote(3, edges, left_edges.at[OWN:2 * OWN, :], peers[3]),
        remote(4, edges, right_edges.at[OWN:2 * OWN, :], peers[4]),
        remote(5, block.at[:, own, upper, :], block.at[:, own, below, :], peers[5]),
        remote(6, edges.at[0:9, :], left_edges.at[below, :], peers[6]),
        remote(7, edges.at[0:9, :], right_edges.at[below, :], peers[7]),
    ]
    from_above, from_side, from_under = sends[0:3], sends[3:5], sends[5:8]
    from_below = from_side + from_under
    totals = [
        remote(8, mine, theirs.at[0], peers[3]),
        remote(9, mine, theirs.at[1], peers[4]),
        remote(10, mine, theirs.at[2], peers[8]),
    ]

    for copy in loads[3:]:
        copy.wait()
    lane = lax.broadcasted_iota(jnp.int32, (OWN, LANES), 1)
    group = ((lane + 16) // 32) % 4
    packed = jnp.zeros((OWN, LANES), jnp.float32)
    ends = [
        jnp.where(lane < 64, block[f, 0, OWN:2 * OWN, :], block[f, tiles_of - 1, OWN:2 * OWN, :]) for f in range(4)]
    for f, piece in enumerate((ends[0], ends[3] * ends[1], ends[3] * ends[2], ends[3])):
        if f:
            piece = pltpu.roll(piece, 32 * f, 1)
        packed = jnp.where(group == f, piece, packed)
    edges[...] = packed
    for k in (1, 2, 0, 3, 4, 6, 7, 5):
        if early[k] is None:
            sends[k].start()
        else:
            pl.when(jnp.logical_not(early[k]))(sends[k].start)

    for copy in loads[:3]:
        copy.wait()
    mine[...] = coefficient_tile(real_s, imag_s, weight_s, poles)
    for k, copy in ((3, totals[0]), (4, totals[1]), (8, totals[2])):
        pl.when(jnp.logical_not(early[k]))(copy.start)

    @pl.when(t == n_tile - 1)
    def _():
        for k, copies in ((5, sends[5:6]), (6, sends[6:7]), (7, sends[7:8]),
                          (3, [sends[3], totals[0]]), (4, [sends[4], totals[1]]), (8, totals[2:])):
            def send(k=k, copies=copies):
                pl.semaphore_wait(ready_sem.at[k], 1)
                for copy in copies:
                    copy.start()
            if k in (5, 6, 7):
                send()
            else:
                pl.when(early[k])(send)

    halo = tiles_of
    tiles = tiles_of + 1
    every = range(tiles)

    def eastward(pieces, step=1, beyond_edge=None):
        edge = lax.broadcasted_iota(jnp.int32, pieces[0].shape, 1) >= LANES - step
        turned = [pltpu.roll(piece, LANES - step, 1) for piece in pieces[:tiles_of]]
        turned.append(pltpu.roll(pieces[halo], LANES - step, 1) if beyond_edge is None else beyond_edge)
        return [jnp.where(edge, turned[(c + 1) % tiles], turned[c]) for c in every]

    def westward(pieces, step=1, beyond_edge=None):
        edge = lax.broadcasted_iota(jnp.int32, pieces[0].shape, 1) < step
        turned = [pltpu.roll(piece, step, 1) for piece in pieces[:tiles_of]]
        turned.append(pltpu.roll(pieces[halo], step, 1) if beyond_edge is None else beyond_edge)
        return [jnp.where(edge, turned[(c - 1) % tiles], turned[c]) for c in every]

    def side(rows):
        wide_lane = lax.broadcasted_iota(jnp.int32, (rows.stop - rows.start, LANES), 1)
        return jnp.where(wide_lane % 32 >= 16, left_edges[rows, :], right_edges[rows, :])

    def side_field(both, f, step=0):
        turn = (2 * LANES - 32 * f - step) % LANES
        return pltpu.roll(both, turn, 1) if turn else both

    def around(pieces, both, f):
        return eastward(pieces, 1, side_field(both, f, 1)), westward(pieces, 1, side_field(both, f, -1))

    def fields(m, f, c, rows):
        start = ((m * 3 + f) * tiles + c) * ROWS
        return chain[start + rows.start:start + rows.stop, :]

    def keep(m, f, c, rows, value):
        start = ((m * 3 + f) * tiles + c) * ROWS
        chain[start + rows.start:start + rows.stop, :] = value

    def prepare(fresh, faces, columns_of, stencil, work):
        both = side(fresh)
        block[0, halo, fresh, :] = both
        block[3, halo, fresh, :] = side_field(both, 3)
        for which in range(2):
            flux[which, halo, fresh, :] = side_field(both, 1 + which)
        both = side(work)
        after_rows = slice(work.start + 1, work.stop + 1)
        before_rows = slice(work.start - 1, work.stop - 1)
        for c in every:
            keep(0, 0, c, fresh, block[0, c, fresh, :])
            if c < tiles_of:
                flux[0, c, fresh, :] = block[3, c, fresh, :] * block[1, c, fresh, :]
                flux[1, c, fresh, :] = block[3, c, fresh, :] * block[2, c, fresh, :]
        for c in every:
            face[c, faces, :] = (block[3, c, faces, :] + block[3, c, faces.start + 1:faces.stop + 1, :]) * 0.125
        here = [block[3, c, columns_of, :] for c in every]
        beside, behind = around(here, both, 3)
        to_north = [(here[c] + beside[c]) * 0.125 for c in every]
        to_south = [(here[c] + behind[c]) * 0.125 for c in every]
        next_north, next_south = eastward(to_north), westward(to_south)
        for c in every:
            north[c, columns_of, :] = to_north[c]
            south[c, columns_of, :] = to_south[c]
            beyond[0, c, columns_of, :] = next_north[c]
            beyond[1, c, columns_of, :] = next_south[c]
        for c in every:
            middle[c, stencil, :] = 2.0 - (
                face[c, stencil, :] + face[c, stencil.start - 1:stencil.stop - 1, :]
                + north[c, stencil, :] + south[c, stencil, :])
        after, before = around([flux[0, c, work, :] for c in every], both, 1)
        after_two, before_two = around([flux[1, c, work, :] for c in every], both, 2)
        for c in every:
            along = flux[0, c, after_rows, :] - flux[0, c, before_rows, :]
            along_two = flux[1, c, after_rows, :] - flux[1, c, before_rows, :]
            keep(0, 1, c, work, 0.5 * (along + (after_two[c] - before_two[c])))
            keep(0, 2, c, work, 0.5 * (along_two - (after[c] - before[c])))

    def advance(m, rows):
        after_rows = slice(rows.start + 1, rows.stop + 1)
        before_rows = slice(rows.start - 1, rows.stop - 1)
        for f in range(3):
            here = [fields(m, f, c, rows) for c in every]
            after, before = eastward(here), westward(here)
            for c in every:
                value = (
                    middle[c, rows, :] * here[c]
                    + face[c, rows, :] * fields(m, f, c, after_rows)
                    + face[c, before_rows, :] * fields(m, f, c, before_rows)
                    + north[c, rows, :] * after[c]
                    + south[c, rows, :] * before[c]
                )
                if m == 0:
                    value = 0.5 * value
                else:
                    value = value - fields(m - 1, f, c, rows)
                keep(m + 1, f, c, rows, value)

    def advance_twice(m, rows, then):
        def beside_rows(window, by):
            return slice(window.start + by, window.stop + by)

        three = range(3)
        up, down = beside_rows(then, 1), beside_rows(then, -1)
        here = [[fields(m, f, c, rows) for c in every] for f in three]
        here_two = [[fields(m, f, c, then) for c in every] for f in three]
        after, before = [eastward(x) for x in here], [westward(x) for x in here]
        plain = [[
            middle[c, then, :] * here_two[f][c]
            + face[c, then, :] * fields(m, f, c, up)
            + face[c, down, :] * fields(m, f, c, down)
            - fields(m - 1, f, c, then)
            for c in every] for f in three]
        plain_after, plain_before = [eastward(x) for x in plain], [westward(x) for x in plain]
        after_two, before_two = [eastward(x, 2) for x in here_two], [westward(x, 2) for x in here_two]
        for f in three:
            for c in every:
                keep(m + 1, f, c, rows, (
                    middle[c, rows, :] * here[f][c]
                    + face[c, rows, :] * fields(m, f, c, beside_rows(rows, 1))
                    + face[c, beside_rows(rows, -1), :] * fields(m, f, c, beside_rows(rows, -1))
                    - fields(m - 1, f, c, rows)
                    + north[c, rows, :] * after[f][c]
                    + south[c, rows, :] * before[f][c]
                ))
        for f in three:
            for c in every:
                to_north, to_south = north[c, then, :], south[c, then, :]
                next_after = (
                    plain_after[f][c] + to_north * here_two[f][c] + beyond[0, c, then, :] * after_two[f][c])
                next_before = (
                    plain_before[f][c] + to_south * here_two[f][c] + beyond[1, c, then, :] * before_two[f][c])
                keep(m + 2, f, c, then, (
                    middle[c, then, :] * fields(m + 1, f, c, then)
                    + face[c, then, :] * fields(m + 1, f, c, up)
                    + face[c, down, :] * fields(m + 1, f, c, down)
                    - here_two[f][c]
                    + to_north * next_after
                    + to_south * next_before
                ))

    def combine(wide, inner):
        for c in every:
            rows = wide
            height = push = lift = None
            for m in range(ITERS):
                for f in range(3):
                    value = fields(m, f, c, rows)
                    one, two = table[3 + f, m:m + 1, :] * value, table[6 + f, m:m + 1, :] * value
                    push, lift = (one, two) if push is None else (push + one, lift + two)
                    if c < tiles_of:
                        part = table[f, m:m + 1, :] * fields(m, f, c, inner)
                        height = part if height is None else height + part
            slope[0, c, rows, :] = push
            slope[1, c, rows, :] = lift
            if c < tiles_of:
                out_ref[0, inner.start - OWN:inner.stop - OWN, c * LANES:(c + 1) * LANES] = height

    def spread_totals():
        for copy in totals:
            copy.wait_recv()
        total = mine[...]
        for d in range(n_pole - 1):
            total = total + theirs[d]
        for index in range(11):
            table[index, :, :] = jnp.broadcast_to(total[:, index:index + 1], (8, LANES))

    def open_seam(seam, away, outside):
        for c in every:
            for which in range(2):
                flux[which, c, outside:outside + 1, :] = jnp.zeros((1, LANES), jnp.float32)

    def gains(seam, away):
        for c in every:
            product = None
            gain[c, 0:1, :] = jnp.ones((1, LANES), jnp.float32)
            for m in range(1, ITERS):
                edge = min(seam + (m - 1) * away, seam + m * away)
                factor = face[c, edge:edge + 1, :]
                product = 0.5 * factor if m == 1 else product * factor
                gain[c, m:m + 1, :] = product

    def close_seam(seam, away, outside):
        last_row = slice(seam + (ITERS - 1) * away, seam + (ITERS - 1) * away + 1)
        for c in every:
            parts = []
            for which in range(2):
                lacking = (0.5 * away) * -flux[which, c, outside:outside + 1, :]
                part = gain[c, :, :] * lacking
                diagonal = pl.ds(((1 + which) * tiles + c) * ROWS + seam, ITERS, stride=3 * tiles * ROWS + away)
                chain[diagonal, :] = chain[diagonal, :] + part
                parts.append(part[ITERS - 1:ITERS, :])
            for potential in range(2):
                slope[potential, c, last_row, :] = (
                    slope[potential, c, last_row, :]
                    + table[3 * potential + 4, ITERS - 1:ITERS, :] * parts[0]
                    + table[3 * potential + 5, ITERS - 1:ITERS, :] * parts[1])

    first_of_plane = lax.rem(t, PLANE) == 0

    @pl.when(first_of_plane)
    def _():
        for copy in from_below:
            copy.wait_recv()
        open_seam(16, 1, 15)
        prepare(slice(16, 48), slice(16, 40), slice(16, 40), slice(16, 40), slice(16, 40))
        for m in range(ITERS - 1):
            advance(m, slice(16, 40) if m < 3 else slice(20, 36))
        gains(16, 1)
        spread_totals()
        combine(slice(23, 39), slice(24, 32))

        @pl.when(t == 0)
        def _():
            def answered(k):
                pl.semaphore_wait(ready_sem.at[k], 1)
                sends[k].start()
            pl.when(p == n_pole - 1)(lambda: answered(6))
            pl.when(p != 0)(lambda: answered(7))
            answered(5)
            pl.when(p != n_pole - 1)(lambda: answered(6))
            pl.when(p == 0)(lambda: answered(7))
        for copy in from_above:
            copy.wait_recv()
        prepare(slice(0, 16), slice(8, 16), slice(8, 16), slice(9, 17), slice(8, 16))
        close_seam(16, 1, 15)
        advance(0, slice(9, 17))
        for m in range(1, ITERS - 1, 2):
            advance_twice(m, slice(9 + m, 17 + m), slice(10 + m, 18 + m))
        combine(slice(15, 23), slice(16, 24))

    @pl.when(jnp.logical_not(first_of_plane))
    def _():
        for copy in from_above + from_side:
            copy.wait_recv()
        open_seam(31, -1, 32)
        prepare(slice(0, 32), slice(7, 31), slice(8, 32), slice(8, 32), slice(8, 32))
        for m in range(ITERS - 1):
            advance(m, slice(8, 32) if m < 3 else slice(12, 28))
        gains(31, -1)
        spread_totals()
        combine(slice(9, 25), slice(16, 24))
        for copy in from_under:
            copy.wait_recv()
        prepare(slice(32, 48), slice(31, 39), slice(32, 40), slice(31, 39), slice(32, 40))
        close_seam(31, -1, 32)
        advance(0, slice(31, 39))
        for m in range(1, ITERS - 1, 2):
            advance_twice(m, slice(31 - m, 39 - m), slice(30 - m, 38 - m))
        combine(slice(25, 33), slice(24, 32))

    rows = slice(OWN, 2 * OWN)
    keep_first, keep_second = table[9, 0:1, :], table[10, 0:1, :]
    here = [slope[0, c, rows, :] for c in every]
    push_after, push_before = eastward(here), westward(here)
    here = [slope[1, c, rows, :] for c in every]
    lift_after, lift_before = eastward(here), westward(here)
    for c in range(tiles_of):
        columns = slice(c * LANES, (c + 1) * LANES)
        east, north_speed = block[1, c, rows, :], block[2, c, rows, :]
        push_along = slope[0, c, OWN + 1:2 * OWN + 1, :] - slope[0, c, OWN - 1:2 * OWN - 1, :]
        lift_along = slope[1, c, OWN + 1:2 * OWN + 1, :] - slope[1, c, OWN - 1:2 * OWN - 1, :]
        out_ref[1, :, columns] = (
            keep_first * east + keep_second * north_speed
            - push_along - (lift_after[c] - lift_before[c]))
        out_ref[2, :, columns] = (
            keep_first * north_speed - keep_second * east
            - (push_after[c] - push_before[c]) + lift_along)

    for copy in sends + totals:
        copy.wait_send()


def shards(state, depth, pole_real, pole_imag, pole_weight):
    fields, rows, columns = state.shape
    poles = pole_real.shape[0]
    tiles = columns // LANES + 1
    n_pole = lax.axis_size("pole")
    f32 = jnp.float32
    return pl.pallas_call(
        kernel,
        out_shape=pltpu.VMEM((3, rows, columns), f32),
        in_specs=[pl.BlockSpec(memory_space=pl.ANY)] * 5,
        out_specs=pl.BlockSpec(memory_space=pltpu.VMEM),
        scratch_shapes=[
            pltpu.VMEM((4, tiles, ROWS, LANES), f32),
            pltpu.VMEM((OWN, LANES), f32),
            pltpu.VMEM((ROWS, LANES), f32),
            pltpu.VMEM((ROWS, LANES), f32),
            pltpu.VMEM((8, LANES), f32),
            pltpu.VMEM((n_pole - 1, 8, LANES), f32),
            pltpu.VMEM((11, 8, LANES), f32),
            pltpu.SMEM((poles,), f32),
            pltpu.SMEM((poles,), f32),
            pltpu.SMEM((2, poles), f32),
            pltpu.VMEM((2, tiles, ROWS, LANES), f32),
            pltpu.VMEM((tiles, ROWS, LANES), f32),
            pltpu.VMEM((tiles, ROWS, LANES), f32),
            pltpu.VMEM((tiles, ROWS, LANES), f32),
            pltpu.VMEM((tiles, ROWS, LANES), f32),
            pltpu.VMEM((ITERS * 3 * tiles * ROWS, LANES), f32),
            pltpu.VMEM((2, tiles, ROWS, LANES), f32),
            pltpu.VMEM((tiles, ITERS, LANES), f32),
            pltpu.VMEM((2, tiles, ROWS, LANES), f32),
            pltpu.SemaphoreType.DMA((3 + 2 * (tiles - 1),)),
            pltpu.SemaphoreType.DMA((11,)),
            pltpu.SemaphoreType.DMA((11,)),
            pltpu.SemaphoreType.REGULAR((len(STEPS),)),
        ],
        compiler_params=pltpu.CompilerParams(collective_id=0, has_side_effects=True),
        name="rexi_step",
    )(state, depth, pole_real, pole_imag, pole_weight)


def solution(mesh):
    return jax.shard_map(
        shards,
        mesh=mesh,
        in_specs=(
            P(None, "tile", "pole"),
            P("tile", "pole"),
            P("pole"),
            P("pole"),
            P(None, "pole"),
        ),
        out_specs=P(None, "tile", "pole"),
        check_vma=False,
    )
```

```python
import jax
import jax.numpy as jnp
from jax import lax
from jax.experimental import pallas as pl
from jax.experimental.pallas import tpu as pltpu
from jax.sharding import PartitionSpec as P

MESH = pl.DeviceIdType.MESH
ITERS = 8
CORIOLIS = 0.7
OWN = 16
ROWS = 3 * OWN
LANES = 128
PLANE = 8
STEPS = ((0, 1), (1, 1), (-1, 1), (1, 0), (-1, 0), (0, -1), (1, -1), (-1, -1), (2, 0))
OPPOSITE = (5, 7, 6, 4, 3, 0, 2, 1, 8)


def times(left, right):
    return (
        left[0] * right[0] - left[1] * right[1],
        left[0] * right[1] + left[1] * right[0],
    )


def inverse(value):
    norm = value[0] * value[0] + value[1] * value[1]
    return (value[0] / norm, -value[1] / norm)


def scaled(factor, value):
    return (factor * value[0], factor * value[1])


def coefficient_tile(real_ref, imag_ref, weight_ref, poles):
    lane = lax.broadcasted_iota(jnp.int32, (8, LANES), 1)
    row = lax.broadcasted_iota(jnp.int32, (8, LANES), 0)
    alpha = [jnp.full((8, LANES), -1.0, jnp.float32), jnp.zeros((8, LANES), jnp.float32)]
    beta = [jnp.zeros((8, LANES), jnp.float32)] * 2
    for k in range(poles):
        here = lane == k
        alpha[0] = jnp.where(here, real_ref[k], alpha[0])
        alpha[1] = jnp.where(here, imag_ref[k], alpha[1])
        beta[0] = jnp.where(here, weight_ref[0, k], beta[0])
        beta[1] = jnp.where(here, weight_ref[1, k], beta[1])
    square = times(alpha, alpha)
    shift = (square[0] + CORIOLIS * CORIOLIS, square[1])
    sigma = ((shift[0] + 8.0) * 0.125, shift[1] * 0.125)
    twice = scaled(2.0, sigma)
    second = [(jnp.ones_like(lane, jnp.float32), jnp.zeros_like(lane, jnp.float32)), twice]
    for _ in range(ITERS - 2):
        product = times(twice, second[-1])
        second.append((product[0] - second[-2][0], product[1] - second[-2][1]))
    product = times(sigma, second[7])
    last = (product[0] - second[6][0], product[1] - second[6][1])
    kappa = scaled(0.125, inverse(last))
    order_real, order_imag = second[7]
    for m in range(1, ITERS):
        order_real = jnp.where(row == m, 2.0 * second[7 - m][0], order_real)
        order_imag = jnp.where(row == m, 2.0 * second[7 - m][1], order_imag)
    over_alpha = inverse(alpha)
    gamma = times(beta, inverse(shift))
    gamma_alpha = times(gamma, alpha)
    weighted = times(kappa, beta)
    gammas = times(kappa, gamma)
    weighted_over = times(weighted, over_alpha)
    gammas_over = times(gammas, over_alpha)
    gammas_alpha = times(gammas, alpha)
    pieces = (
        times(weighted_over, shift),
        scaled(-1.0, weighted),
        scaled(-CORIOLIS, weighted_over),
        scaled(0.5, weighted),
        scaled(-0.5, gammas_alpha),
        scaled(-0.5 * CORIOLIS, gammas),
        scaled(0.5 * CORIOLIS, weighted_over),
        scaled(-0.5 * CORIOLIS, gammas),
        scaled(-0.5 * CORIOLIS * CORIOLIS, gammas_over),
    )
    sums = [piece[0] * order_real - piece[1] * order_imag for piece in pieces]
    sums += [gamma_alpha[0], CORIOLIS * gamma[0]]
    tile = jnp.zeros((8, LANES), jnp.float32)
    for index, value in enumerate(sums):
        tile = jnp.where(lane == index, jnp.sum(value, axis=1, keepdims=True), tile)
    return tile


def waits_for(step, p, t, n_pole, n_tile):
    dp, dt = step
    last = t == n_tile - 1
    if dt < 0:
        return jnp.logical_or(t == 0, last)
    if dt > 0:
        return None
    return jnp.logical_and(last, {1: p != n_pole - 1, -1: p == 0, 2: p < n_pole // 2}[dp])


def heard_later(step, p, t, n_pole, n_tile):
    dp, dt = step
    last = t == n_tile - 1
    if dt > 0:
        return jnp.logical_or(last, t == n_tile - 2)
    if dt < 0:
        return None
    return jnp.logical_and(last, {1: p == n_pole - 1, -1: p != 0, 2: p >= n_pole // 2}[dp])


def kernel(
    state_ref, depth_ref, real_ref, imag_ref, weight_ref, out_ref,
    block, edges, left_edges, right_edges, mine, theirs, table,
    real_s, imag_s, weight_s,
    flux, face, north, south, middle, chain, slope, gain, beyond,
    load_sem, send_sem, recv_sem, ready_sem,
):
    poles = real_s.shape[0]
    tiles_of = state_ref.shape[2] // LANES
    p, t = lax.axis_index("pole"), lax.axis_index("tile")
    n_pole, n_tile = lax.axis_size("pole"), lax.axis_size("tile")
    peers = [(lax.rem(p + dp + n_pole, n_pole), lax.rem(t + dt + n_tile, n_tile)) for dp, dt in STEPS]
    early = [waits_for(step, p, t, n_pole, n_tile) for step in STEPS]
    late = [heard_later(step, p, t, n_pole, n_tile) for step in STEPS]

    loads = [
        pltpu.make_async_copy(real_ref, real_s, load_sem.at[0]),
        pltpu.make_async_copy(imag_ref, imag_s, load_sem.at[1]),
        pltpu.make_async_copy(weight_ref, weight_s, load_sem.at[2]),
    ]
    for c in range(tiles_of):
        columns = pl.ds(c * LANES, LANES)
        loads.append(pltpu.make_async_copy(
            state_ref.at[:, :, columns], block.at[0:3, c, OWN:2 * OWN, :], load_sem.at[3 + 2 * c]))
        loads.append(pltpu.make_async_copy(
            depth_ref.at[:, columns], block.at[3, c, OWN:2 * OWN, :], load_sem.at[4 + 2 * c]))
    for copy in loads[3:] + loads[:3]:
        copy.start()

    barrier = pltpu.get_barrier_semaphore()
    expected = jnp.int32(len(STEPS))
    for k, to in enumerate(peers):
        if early[k] is not None:
            expected = expected - early[k].astype(jnp.int32)

        def greet(to=to):
            pl.semaphore_signal(barrier, inc=1, device_id=to, device_id_type=MESH)
        if late[k] is None:
            greet()
        else:
            pl.when(jnp.logical_not(late[k]))(greet)
    pl.semaphore_wait(barrier, expected)
    for k, to in enumerate(peers):
        if late[k] is not None:
            @pl.when(late[k])
            def answer(k=k, to=to):
                pl.semaphore_signal(ready_sem.at[OPPOSITE[k]], inc=1, device_id=to, device_id_type=MESH)

    def remote(index, source, target, to):
        return pltpu.make_async_remote_copy(
            src_ref=source, dst_ref=target, send_sem=send_sem.at[index], recv_sem=recv_sem.at[index],
            device_id=to, device_id_type=MESH)

    own = pl.ds(0, tiles_of)
    lower, upper = slice(23, 32), slice(16, 25)
    above, below = slice(7, 16), slice(32, 41)
    sends = [
        remote(0, block.at[:, own, lower, :], block.at[:, own, above, :], peers[0]),
        remote(1, edges.at[7:16, :], left_edges.at[above, :], peers[1]),
        remote(2, edges.at[7:16, :], right_edges.at[above, :], peers[2]),
        remote(3, edges, left_edges.at[OWN:2 * OWN, :], peers[3]),
        remote(4, edges, right_edges.at[OWN:2 * OWN, :], peers[4]),
        remote(5, block.at[:, own, upper, :], block.at[:, own, below, :], peers[5]),
        remote(6, edges.at[0:9, :], left_edges.at[below, :], peers[6]),
        remote(7, edges.at[0:9, :], right_edges.at[below, :], peers[7]),
    ]
    from_above, from_side, from_under = sends[0:3], sends[3:5], sends[5:8]
    from_below = from_side + from_under
    totals = [
        remote(8, mine, theirs.at[0], peers[3]),
        remote(9, mine, theirs.at[1], peers[4]),
        remote(10, mine, theirs.at[2], peers[8]),
    ]

    for copy in loads[3:]:
        copy.wait()
    lane = lax.broadcasted_iota(jnp.int32, (OWN, LANES), 1)
    group = ((lane + 16) // 32) % 4
    packed = jnp.zeros((OWN, LANES), jnp.float32)
    ends = [
        jnp.where(lane < 64, block[f, 0, OWN:2 * OWN, :], block[f, tiles_of - 1, OWN:2 * OWN, :]) for f in range(4)]
    for f, piece in enumerate((ends[0], ends[3] * ends[1], ends[3] * ends[2], ends[3])):
        if f:
            piece = pltpu.roll(piece, 32 * f, 1)
        packed = jnp.where(group == f, piece, packed)
    edges[...] = packed
    for k in (1, 2, 0, 3, 4, 6, 7, 5):
        if early[k] is None:
            sends[k].start()
        else:
            pl.when(jnp.logical_not(early[k]))(sends[k].start)

    for copy in loads[:3]:
        copy.wait()
    mine[...] = coefficient_tile(real_s, imag_s, weight_s, poles)
    for k, copy in ((3, totals[0]), (4, totals[1]), (8, totals[2])):
        pl.when(jnp.logical_not(early[k]))(copy.start)

    @pl.when(t == n_tile - 1)
    def _():
        for k, copies in ((5, sends[5:6]), (6, sends[6:7]), (7, sends[7:8]),
                          (3, [sends[3], totals[0]]), (4, [sends[4], totals[1]]), (8, totals[2:])):
            def send(k=k, copies=copies):
                pl.semaphore_wait(ready_sem.at[k], 1)
                for copy in copies:
                    copy.start()
            if k in (5, 6, 7):
                send()
            else:
                pl.when(early[k])(send)

    halo = tiles_of
    tiles = tiles_of + 1
    every = range(tiles)

    def eastward(pieces, step=1, beyond_edge=None):
        edge = lax.broadcasted_iota(jnp.int32, pieces[0].shape, 1) >= LANES - step
        turned = [pltpu.roll(piece, LANES - step, 1) for piece in pieces[:tiles_of]]
        turned.append(pltpu.roll(pieces[halo], LANES - step, 1) if beyond_edge is None else beyond_edge)
        return [jnp.where(edge, turned[(c + 1) % tiles], turned[c]) for c in every]

    def westward(pieces, step=1, beyond_edge=None):
        edge = lax.broadcasted_iota(jnp.int32, pieces[0].shape, 1) < step
        turned = [pltpu.roll(piece, step, 1) for piece in pieces[:tiles_of]]
        turned.append(pltpu.roll(pieces[halo], step, 1) if beyond_edge is None else beyond_edge)
        return [jnp.where(edge, turned[(c - 1) % tiles], turned[c]) for c in every]

    def side(rows):
        wide_lane = lax.broadcasted_iota(jnp.int32, (rows.stop - rows.start, LANES), 1)
        return jnp.where(wide_lane % 32 >= 16, left_edges[rows, :], right_edges[rows, :])

    def side_field(both, f, step=0):
        turn = (2 * LANES - 32 * f - step) % LANES
        return pltpu.roll(both, turn, 1) if turn else both

    def around(pieces, both, f):
        return eastward(pieces, 1, side_field(both, f, 1)), westward(pieces, 1, side_field(both, f, -1))

    def fields(m, f, c, rows):
        start = ((m * 3 + f) * tiles + c) * ROWS
        return chain[start + rows.start:start + rows.stop, :]

    def keep(m, f, c, rows, value):
        start = ((m * 3 + f) * tiles + c) * ROWS
        chain[start + rows.start:start + rows.stop, :] = value

    def prepare(fresh, faces, columns_of, stencil, work):
        both = side(fresh)
        block[0, halo, fresh, :] = both
        block[3, halo, fresh, :] = side_field(both, 3)
        for which in range(2):
            flux[which, halo, fresh, :] = side_field(both, 1 + which)
        both = side(work)
        after_rows = slice(work.start + 1, work.stop + 1)
        before_rows = slice(work.start - 1, work.stop - 1)
        for c in every:
            keep(0, 0, c, fresh, block[0, c, fresh, :])
            if c < tiles_of:
                flux[0, c, fresh, :] = block[3, c, fresh, :] * block[1, c, fresh, :]
                flux[1, c, fresh, :] = block[3, c, fresh, :] * block[2, c, fresh, :]
        for c in every:
            face[c, faces, :] = (block[3, c, faces, :] + block[3, c, faces.start + 1:faces.stop + 1, :]) * 0.125
        here = [block[3, c, columns_of, :] for c in every]
        beside, behind = around(here, both, 3)
        to_north = [(here[c] + beside[c]) * 0.125 for c in every]
        to_south = [(here[c] + behind[c]) * 0.125 for c in every]
        next_north, next_south = eastward(to_north), westward(to_south)
        for c in every:
            north[c, columns_of, :] = to_north[c]
            south[c, columns_of, :] = to_south[c]
            beyond[0, c, columns_of, :] = next_north[c]
            beyond[1, c, columns_of, :] = next_south[c]
        for c in every:
            middle[c, stencil, :] = 2.0 - (
                face[c, stencil, :] + face[c, stencil.start - 1:stencil.stop - 1, :]
                + north[c, stencil, :] + south[c, stencil, :])
        after, before = around([flux[0, c, work, :] for c in every], both, 1)
        after_two, before_two = around([flux[1, c, work, :] for c in every], both, 2)
        for c in every:
            along = flux[0, c, after_rows, :] - flux[0, c, before_rows, :]
            along_two = flux[1, c, after_rows, :] - flux[1, c, before_rows, :]
            keep(0, 1, c, work, 0.5 * (along + (after_two[c] - before_two[c])))
            keep(0, 2, c, work, 0.5 * (along_two - (after[c] - before[c])))

    def advance(m, rows):
        after_rows = slice(rows.start + 1, rows.stop + 1)
        before_rows = slice(rows.start - 1, rows.stop - 1)
        for f in range(3):
            here = [fields(m, f, c, rows) for c in every]
            after, before = eastward(here), westward(here)
            for c in every:
                value = (
                    middle[c, rows, :] * here[c]
                    + face[c, rows, :] * fields(m, f, c, after_rows)
                    + face[c, before_rows, :] * fields(m, f, c, before_rows)
                    + north[c, rows, :] * after[c]
                    + south[c, rows, :] * before[c]
                )
                if m == 0:
                    value = 0.5 * value
                else:
                    value = value - fields(m - 1, f, c, rows)
                keep(m + 1, f, c, rows, value)

    def advance_twice(m, rows, then):
        def beside_rows(window, by):
            return slice(window.start + by, window.stop + by)

        for f in range(3):
            here = [fields(m, f, c, rows) for c in every]
            after, before = eastward(here), westward(here)
            here_two = [fields(m, f, c, then) for c in every]
            after_two, before_two = eastward(here_two, 2), westward(here_two, 2)
            plain = [
                middle[c, then, :] * here_two[c]
                + face[c, then, :] * fields(m, f, c, beside_rows(then, 1))
                + face[c, beside_rows(then, -1), :] * fields(m, f, c, beside_rows(then, -1))
                - fields(m - 1, f, c, then)
                for c in every
            ]
            plain_after, plain_before = eastward(plain), westward(plain)
            for c in every:
                keep(m + 1, f, c, rows, (
                    middle[c, rows, :] * here[c]
                    + face[c, rows, :] * fields(m, f, c, beside_rows(rows, 1))
                    + face[c, beside_rows(rows, -1), :] * fields(m, f, c, beside_rows(rows, -1))
                    - fields(m - 1, f, c, rows)
                    + north[c, rows, :] * after[c]
                    + south[c, rows, :] * before[c]
                ))
            for c in every:
                to_north, to_south = north[c, then, :], south[c, then, :]
                next_after = plain_after[c] + to_north * here_two[c] + beyond[0, c, then, :] * after_two[c]
                next_before = plain_before[c] + to_south * here_two[c] + beyond[1, c, then, :] * before_two[c]
                keep(m + 2, f, c, then, (
                    middle[c, then, :] * fields(m + 1, f, c, then)
                    + face[c, then, :] * fields(m + 1, f, c, beside_rows(then, 1))
                    + face[c, beside_rows(then, -1), :] * fields(m + 1, f, c, beside_rows(then, -1))
                    - here_two[c]
                    + to_north * next_after
                    + to_south * next_before
                ))

    def combine(wide, inner):
        for c in every:
            rows = wide
            height = push = lift = None
            for m in range(ITERS):
                for f in range(3):
                    value = fields(m, f, c, rows)
                    one, two = table[3 + f, m:m + 1, :] * value, table[6 + f, m:m + 1, :] * value
                    push, lift = (one, two) if push is None else (push + one, lift + two)
                    if c < tiles_of:
                        part = table[f, m:m + 1, :] * fields(m, f, c, inner)
                        height = part if height is None else height + part
            slope[0, c, rows, :] = push
            slope[1, c, rows, :] = lift
            if c < tiles_of:
                out_ref[0, inner.start - OWN:inner.stop - OWN, c * LANES:(c + 1) * LANES] = height

    def spread_totals():
        for copy in totals:
            copy.wait_recv()
        total = mine[...]
        for d in range(n_pole - 1):
            total = total + theirs[d]
        for index in range(11):
            table[index, :, :] = jnp.broadcast_to(total[:, index:index + 1], (8, LANES))

    def open_seam(seam, away, outside):
        for c in every:
            for which in range(2):
                flux[which, c, outside:outside + 1, :] = jnp.zeros((1, LANES), jnp.float32)

    def gains(seam, away):
        for c in every:
            product = None
            gain[c, 0:1, :] = jnp.ones((1, LANES), jnp.float32)
            for m in range(1, ITERS):
                edge = min(seam + (m - 1) * away, seam + m * away)
                factor = face[c, edge:edge + 1, :]
                product = 0.5 * factor if m == 1 else product * factor
                gain[c, m:m + 1, :] = product

    def close_seam(seam, away, outside):
        last_row = slice(seam + (ITERS - 1) * away, seam + (ITERS - 1) * away + 1)
        for c in every:
            parts = []
            for which in range(2):
                lacking = (0.5 * away) * -flux[which, c, outside:outside + 1, :]
                part = gain[c, :, :] * lacking
                diagonal = pl.ds(((1 + which) * tiles + c) * ROWS + seam, ITERS, stride=3 * tiles * ROWS + away)
                chain[diagonal, :] = chain[diagonal, :] + part
                parts.append(part[ITERS - 1:ITERS, :])
            for potential in range(2):
                slope[potential, c, last_row, :] = (
                    slope[potential, c, last_row, :]
                    + table[3 * potential + 4, ITERS - 1:ITERS, :] * parts[0]
                    + table[3 * potential + 5, ITERS - 1:ITERS, :] * parts[1])

    first_of_plane = lax.rem(t, PLANE) == 0

    @pl.when(first_of_plane)
    def _():
        for copy in from_below:
            copy.wait_recv()
        open_seam(16, 1, 15)
        prepare(slice(16, 48), slice(16, 40), slice(16, 40), slice(16, 40), slice(16, 40))
        for m in range(ITERS - 1):
            advance(m, slice(16, 40) if m < 3 else slice(20, 36))
        gains(16, 1)
        spread_totals()
        combine(slice(23, 39), slice(24, 32))

        @pl.when(t == 0)
        def _():
            def answered(k):
                pl.semaphore_wait(ready_sem.at[k], 1)
                sends[k].start()
            pl.when(p == n_pole - 1)(lambda: answered(6))
            pl.when(p != 0)(lambda: answered(7))
            answered(5)
            pl.when(p != n_pole - 1)(lambda: answered(6))
            pl.when(p == 0)(lambda: answered(7))
        for copy in from_above:
            copy.wait_recv()
        prepare(slice(0, 16), slice(8, 16), slice(8, 16), slice(9, 17), slice(8, 16))
        close_seam(16, 1, 15)
        advance(0, slice(9, 17))
        for m in range(1, ITERS - 1, 2):
            advance_twice(m, slice(9 + m, 17 + m), slice(10 + m, 18 + m))
        combine(slice(15, 23), slice(16, 24))

    @pl.when(jnp.logical_not(first_of_plane))
    def _():
        for copy in from_above + from_side:
            copy.wait_recv()
        open_seam(31, -1, 32)
        prepare(slice(0, 32), slice(7, 31), slice(8, 32), slice(8, 32), slice(8, 32))
        for m in range(ITERS - 1):
            advance(m, slice(8, 32) if m < 3 else slice(12, 28))
        gains(31, -1)
        spread_totals()
        combine(slice(9, 25), slice(16, 24))
        for copy in from_under:
            copy.wait_recv()
        prepare(slice(32, 48), slice(31, 39), slice(32, 40), slice(31, 39), slice(32, 40))
        close_seam(31, -1, 32)
        advance(0, slice(31, 39))
        for m in range(1, ITERS - 1, 2):
            advance_twice(m, slice(31 - m, 39 - m), slice(30 - m, 38 - m))
        combine(slice(25, 33), slice(24, 32))

    rows = slice(OWN, 2 * OWN)
    keep_first, keep_second = table[9, 0:1, :], table[10, 0:1, :]
    here = [slope[0, c, rows, :] for c in every]
    push_after, push_before = eastward(here), westward(here)
    here = [slope[1, c, rows, :] for c in every]
    lift_after, lift_before = eastward(here), westward(here)
    for c in range(tiles_of):
        columns = slice(c * LANES, (c + 1) * LANES)
        east, north_speed = block[1, c, rows, :], block[2, c, rows, :]
        push_along = slope[0, c, OWN + 1:2 * OWN + 1, :] - slope[0, c, OWN - 1:2 * OWN - 1, :]
        lift_along = slope[1, c, OWN + 1:2 * OWN + 1, :] - slope[1, c, OWN - 1:2 * OWN - 1, :]
        out_ref[1, :, columns] = (
            keep_first * east + keep_second * north_speed
            - push_along - (lift_after[c] - lift_before[c]))
        out_ref[2, :, columns] = (
            keep_first * north_speed - keep_second * east
            - (push_after[c] - push_before[c]) + lift_along)

    for copy in sends + totals:
        copy.wait_send()


def shards(state, depth, pole_real, pole_imag, pole_weight):
    fields, rows, columns = state.shape
    poles = pole_real.shape[0]
    tiles = columns // LANES + 1
    n_pole = lax.axis_size("pole")
    f32 = jnp.float32
    return pl.pallas_call(
        kernel,
        out_shape=pltpu.VMEM((3, rows, columns), f32),
        in_specs=[pl.BlockSpec(memory_space=pl.ANY)] * 5,
        out_specs=pl.BlockSpec(memory_space=pltpu.VMEM),
        scratch_shapes=[
            pltpu.VMEM((4, tiles, ROWS, LANES), f32),
            pltpu.VMEM((OWN, LANES), f32),
            pltpu.VMEM((ROWS, LANES), f32),
            pltpu.VMEM((ROWS, LANES), f32),
            pltpu.VMEM((8, LANES), f32),
            pltpu.VMEM((n_pole - 1, 8, LANES), f32),
            pltpu.VMEM((11, 8, LANES), f32),
            pltpu.SMEM((poles,), f32),
            pltpu.SMEM((poles,), f32),
            pltpu.SMEM((2, poles), f32),
            pltpu.VMEM((2, tiles, ROWS, LANES), f32),
            pltpu.VMEM((tiles, ROWS, LANES), f32),
            pltpu.VMEM((tiles, ROWS, LANES), f32),
            pltpu.VMEM((tiles, ROWS, LANES), f32),
            pltpu.VMEM((tiles, ROWS, LANES), f32),
            pltpu.VMEM((ITERS * 3 * tiles * ROWS, LANES), f32),
            pltpu.VMEM((2, tiles, ROWS, LANES), f32),
            pltpu.VMEM((tiles, ITERS, LANES), f32),
            pltpu.VMEM((2, tiles, ROWS, LANES), f32),
            pltpu.SemaphoreType.DMA((3 + 2 * (tiles - 1),)),
            pltpu.SemaphoreType.DMA((11,)),
            pltpu.SemaphoreType.DMA((11,)),
            pltpu.SemaphoreType.REGULAR((len(STEPS),)),
        ],
        compiler_params=pltpu.CompilerParams(collective_id=0, has_side_effects=True),
        name="rexi_step",
    )(state, depth, pole_real, pole_imag, pole_weight)


def solution(mesh):
    return jax.shard_map(
        shards,
        mesh=mesh,
        in_specs=(
            P(None, "tile", "pole"),
            P("tile", "pole"),
            P("pole"),
            P("pole"),
            P(None, "pole"),
        ),
        out_specs=P(None, "tile", "pole"),
        check_vma=False,
    )
```
